8 devices in a mesh: ens: 2 (over z, y), feat: 4 (over x, core).
Axes of the slice: x: 2, y: 2, z: 1, core: 2. Of those that a mesh axis runs over, the one named last changes fastest.
Arguments:
- particles: float32 [1024, 32768], P('ens', 'feat'), parts along dimension 0
- prec_diag: float32 [65536], P(('ens', 'feat')), parts along dimension 0
- low_factor: bfloat16 [65536, 16], P(('ens', 'feat')), parts along dimension 0
- prior_mean: float32 [65536], P(('ens', 'feat')), parts along dimension 0
- data_mat: bfloat16 [2048, 32768], P('ens', 'feat'), parts along dimension 0
- labels: int32 [2048], P('ens'), parts along dimension 0
Outputs:
- output: float32 [1024, 32768], P('ens', 'feat'), parts along dimension 0
There are 2 independent parts. The reference program is written for one: setup_inputs(seed, part) draws one part's arguments, and reference() takes and returns one part's arrays. A program takes and returns all parts, laid end to end along the dimension named above; each array names one.
All inputs are finite; a program needn't handle non-finite values.
Results may differ from the reference program's by a relative error of at most 0.001.
Values are sent between devices in bfloat16 or wider.
A program may use at most 1 GiB of HBM per device.

```python
import math
import jax
import jax.numpy as jnp

FEAT_DIM = 32768
LOW_RANK = 16
PARTICLES = 512
DATA_ROWS = 1024
NUM_STEPS = 3


def setup_inputs(seed: int = 0, part: int = 0) -> dict:
    base_key = jax.random.fold_in(jax.random.key(seed), part)
    sub_keys = jax.random.split(base_key, 8)
    common = jax.random.normal(sub_keys[0], (1, FEAT_DIM), jnp.float32)
    spread = jax.random.uniform(sub_keys[1], (PARTICLES, 1), jnp.float32, 0.5, 1.5)
    noise_mat = jax.random.normal(sub_keys[2], (PARTICLES, FEAT_DIM), jnp.float32)
    particles = common + spread * noise_mat
    prec_diag = jnp.exp(jax.random.uniform(sub_keys[3], (FEAT_DIM,), jnp.float32, -1.0, 1.0)) / FEAT_DIM
    u_scale = 1.1 * (FEAT_DIM * math.sqrt(LOW_RANK * FEAT_DIM)) ** -0.5
    low_factor = (jax.random.normal(sub_keys[4], (FEAT_DIM, LOW_RANK), jnp.float32) * u_scale).astype(jnp.bfloat16)
    prior_mean = 0.5 * jax.random.normal(sub_keys[5], (FEAT_DIM,), jnp.float32)
    data_scale = 1.5 / math.sqrt(FEAT_DIM)
    data_mat = (jax.random.normal(sub_keys[6], (DATA_ROWS, FEAT_DIM), jnp.float32) * data_scale).astype(jnp.bfloat16)
    labels = jax.random.randint(sub_keys[7], (DATA_ROWS,), 0, 2, jnp.int32)
    return {"particles": particles, "prec_diag": prec_diag, "low_factor": low_factor,
            "prior_mean": prior_mean, "data_mat": data_mat, "labels": labels}


def reference(particles, prec_diag, low_factor, prior_mean, data_mat, labels):
    band_width = 2.0 * FEAT_DIM
    step_size = FEAT_DIM / 4.0
    lik_weight = 2.0 / math.sqrt(DATA_ROWS * FEAT_DIM)
    targets = labels.astype(jnp.float32)[None, :]
    state = particles
    for step_idx in range(NUM_STEPS):
        part_bf = state.astype(jnp.bfloat16)
        centred = state - prior_mean
        projected = jnp.dot(centred.astype(jnp.bfloat16), low_factor, preferred_element_type=jnp.float32)
        gram_mat = jnp.dot(part_bf, part_bf.T, preferred_element_type=jnp.float32)
        sq_norm = jnp.diagonal(gram_mat)
        sq_dist = jnp.maximum(sq_norm[:, None] + sq_norm[None, :] - 2.0 * gram_mat, 0.0)
        kernel = jnp.exp(-sq_dist / band_width)
        logits = jnp.dot(part_bf, data_mat.T, preferred_element_type=jnp.float32)
        residual = targets - jax.nn.sigmoid(logits)
        low_rank = jnp.dot(projected.astype(jnp.bfloat16), low_factor.T, preferred_element_type=jnp.float32)
        lik_term = jnp.dot(residual.astype(jnp.bfloat16), data_mat, preferred_element_type=jnp.float32)
        log_grad = lik_weight * lik_term - centred * prec_diag - low_rank
        kern_bf = kernel.astype(jnp.bfloat16)
        driving = jnp.dot(kern_bf, log_grad.astype(jnp.bfloat16), preferred_element_type=jnp.float32)
        pulled = jnp.dot(kern_bf, part_bf, preferred_element_type=jnp.float32)
        row_sum = jnp.sum(kernel, axis=1, keepdims=True)
        update_dir = (driving + (2.0 / band_width) * (row_sum * state - pulled)) / PARTICLES
        state = state + step_size * update_dir
    return state
```

```python
import functools
import math
import jax
import jax.numpy as jnp
from jax import lax
from jax.experimental import pallas as pl
from jax.experimental.pallas import tpu as pltpu
from jax.sharding import PartitionSpec as P

NUM_STEPS = 3
NT = (((1,), (1,)), ((), ()))
F32 = jnp.float32
BF16 = jnp.bfloat16
N = 512
HB = 256
D = 8192
M = 1024
CW = 2048
SW = 512
NC = D // CW
VMEM_LIMIT = 67_043_328


def run_kernel(consts, th_hbm, lam_ref, ut_ref, mu_ref, a_hbm, y_ref,
               th_out, s_out, k_out, kv_out,
               th, a, tb, sbuf, zbuf, ra, snd, rb, rbuf, kx, kv, qacc, qall, dgs, dall, qt,
               ld_sem, a_sem, out_sem, as_sem, ar_sem, bs_sem, br_sem, cs_sem, cr_sem, ds_sem, dr_sem,
               ks_sem, kr_sem, ls_sem, lr_sem, qs_sem, qr_sem, gs_sem, gr_sem):
    lik_weight, inv_band, two_over_band, gain = consts
    me = lax.axis_index("feat")
    xx = me // 2
    cc = me % 2
    sib = xx * 2 + (1 - cc)
    far = (1 - xx) * 2 + cc
    diag_dev = (1 - xx) * 2 + (1 - cc)

    def rows_of(idx):
        return jnp.where(idx < 4, idx // 2, idx - 4) * HB

    def remote(src, dst, ssem, rsem, dev):
        return pltpu.make_async_remote_copy(
            src_ref=src, dst_ref=dst, send_sem=ssem, recv_sem=rsem,
            device_id={"feat": dev}, device_id_type=pl.DeviceIdType.MESH)

    def copy_a(idx):
        return remote(zbuf.at[idx, pl.ds((1 - cc) * 128, 128), :], ra.at[idx], as_sem.at[idx], ar_sem.at[idx], sib)

    def copy_b(idx):
        return remote(snd.at[idx], rb.at[idx], bs_sem.at[idx], br_sem.at[idx], far)

    def z_region(idx, first, count):
        if isinstance(idx, int):
            b, j = divmod(idx, 2)
        else:
            b, j = idx // 2, idx % 2
        return rbuf.at[pl.ds(b * HB + first, count), pl.ds(pl.multiple_of(j * 512, 512), 512)]

    def region(idx, first, count):
        if idx >= 4:
            return kx.at[pl.ds((idx - 4) * HB + first, count), pl.ds(0, 512)]
        return z_region(idx, first, count)

    def copy_c(idx):
        r = region(idx, cc * 128 + xx * 64, 64)
        return remote(r, r, cs_sem.at[idx], cr_sem.at[idx], far)

    def copy_d(idx):
        r = region(idx, cc * 128, 128)
        return remote(r, r, ds_sem.at[idx], dr_sem.at[idx], sib)

    def copy_ck(idx):
        r = kv.at[pl.ds((idx - 4) * HB + cc * 128 + xx * 64, 64), :]
        return remote(r, r, ks_sem.at[idx - 4], kr_sem.at[idx - 4], far)

    def copy_dk(idx):
        r = kv.at[pl.ds((idx - 4) * HB + cc * 128, 128), :]
        return remote(r, r, ls_sem.at[idx - 4], lr_sem.at[idx - 4], sib)

    def stage_a(idx):
        copy_a(idx).start()

    def stage_b(idx):
        copy_a(idx).wait_recv()
        o = (1 - xx) * 64
        snd[idx] = zbuf[idx, pl.ds(cc * 128 + o, 64), :] + ra[idx, pl.ds(o, 64), :]
        copy_b(idx).start()

    def stage_c(idx):
        copy_b(idx).wait_recv()
        o = xx * 64
        val = (zbuf[idx, pl.ds(cc * 128 + o, 64), :] + ra[idx, pl.ds(o, 64), :]) + rb[idx]
        if idx < 4:
            j = idx % 2
            res = y_ref[:, j * 512:(j + 1) * 512] - jax.nn.sigmoid(val)
            rbuf[pl.ds((idx // 2) * HB + cc * 128 + o, 64), j * 512:(j + 1) * 512] = res.astype(BF16)
        else:
            if idx == 4:
                for p in range(3):
                    small_g(p).wait_recv()
            nj = ((dall[2 * xx] + dall[2 * xx + 1]) + (dall[2 * (1 - xx)] + dall[2 * (1 - xx) + 1]))[0:1, :]
            first = (idx - 4) * HB + cc * 128 + o
            rid = lax.broadcasted_iota(jnp.int32, (64, N), 0) + first
            cid = lax.broadcasted_iota(jnp.int32, (64, N), 1)
            ni = jnp.sum(jnp.where(rid == cid, nj, 0.0), axis=1, keepdims=True)
            dist = jnp.maximum(ni + nj - 2.0 * val, 0.0)
            kern = jnp.exp(-dist * inv_band)
            kx[pl.ds(first, 64), 0:512] = kern.astype(BF16)
            kv[pl.ds(first, 64), :] = jnp.broadcast_to(jnp.sum(kern, axis=1, keepdims=True), (64, 128))
            copy_ck(idx).start()
        copy_c(idx).start()
        copy_a(idx).wait_send()
        copy_b(idx).wait_send()

    def stage_d(idx):
        copy_c(idx).wait()
        copy_d(idx).start()
        if idx >= 4:
            copy_ck(idx).wait()
            copy_dk(idx).start()

    def stage_e(idx):
        copy_d(idx).wait()
        if idx >= 4:
            copy_dk(idx).wait()

    peers = (sib, far, diag_dev)
    def small_q(p):
        return remote(qall.at[me], qall.at[me], qs_sem.at[p], qr_sem.at[p], peers[p])

    def small_g(p):
        return remote(dall.at[me], dall.at[me], gs_sem.at[p], gr_sem.at[p], peers[p])

    def load_th(b, c):
        v = (pl.ds(b * HB, HB), pl.ds(pl.multiple_of(c * CW, CW), CW))
        return pltpu.make_async_copy(th_hbm.at[v], th.at[v], ld_sem.at[b * NC + c])

    def load_a(j):
        v = (pl.ds(j * 512, 512), slice(None))
        return pltpu.make_async_copy(a_hbm.at[v], a.at[v], a_sem.at[j])

    for c in range(NC):
        load_th(0, c).start()
    for j in range(2):
        load_a(j).start()
    for c in range(NC):
        load_th(1, c).start()

    barrier = pltpu.get_barrier_semaphore()
    for p in peers:
        pl.semaphore_signal(barrier, inc=1, device_id={"feat": p}, device_id_type=pl.DeviceIdType.MESH)
    pl.semaphore_wait(barrier, 3)

    def out_theta():
        return pltpu.make_async_copy(th, th_out, out_sem.at[0])

    def out_s(b):
        v = (pl.ds(b * HB, HB), slice(None))
        return pltpu.make_async_copy(sbuf.at[v], s_out.at[v], out_sem.at[1 + b])

    def step(s, carry):
        par = s % 2
        old = 1 - par
        new_rows = (512 * par, HB)
        obase = 256 * old

        def project(b, c0, xb):
            part = lax.dot_general(ut_ref[:, c0], xb, NT, preferred_element_type=F32)
            qacc[:, b * HB:(b + 1) * HB] += part

        def load_phase(b):
            def body(c, carry):
                load_th(b, c).wait()
                for i in range(CW // SW):
                    cs = pl.ds(pl.multiple_of(c * CW + i * SW, SW), SW)
                    t = th[b * HB:(b + 1) * HB, cs]
                    tb[pl.ds(pl.multiple_of(new_rows[b], HB), HB), cs] = t.astype(BF16)
                    project(b, cs, (t - mu_ref[:, cs]).astype(BF16))
                return carry
            lax.fori_loop(0, NC, body, 0)

        def update_phase(b):
            def body(c, carry):
                if b == 1:
                    k_events(c)
                kb = kx[b * HB:(b + 1) * HB, 0:512]
                kt = kx[b * HB:(b + 1) * HB, pl.ds(pl.multiple_of(obase, HB), 512)]
                kvb = kv[b * HB:(b + 1) * HB, 0:1]
                for i in range(CW // SW):
                    cs = pl.ds(pl.multiple_of(c * CW + i * SW, SW), SW)
                    drive = jnp.dot(kb, sbuf[:, cs], preferred_element_type=F32)
                    pull = jnp.dot(kt, tb[pl.ds(pl.multiple_of(obase, HB), 512), cs], preferred_element_type=F32)
                    t = th[b * HB:(b + 1) * HB, cs]
                    t = t + gain * (drive + two_over_band * (kvb * t - pull))
                    th[b * HB:(b + 1) * HB, cs] = t
                    tb[pl.ds(pl.multiple_of(new_rows[b], HB), HB), cs] = t.astype(BF16)
                    project(b, cs, (t - mu_ref[:, cs]).astype(BF16))
                return carry
            lax.fori_loop(0, NC, body, 0)

        def k_events(c):
            @pl.when(c == 0)
            def _():
                stage_b(0)

            @pl.when(c == 1)
            def _():
                stage_b(1)

            @pl.when(c == 2)
            def _():
                stage_c(0)

            @pl.when(c == 3)
            def _():
                stage_c(1)

        qacc[...] = jnp.zeros_like(qacc)
        for b in range(2):
            @pl.when(s == 0)
            def _():
                load_phase(b)
                if b == 1:
                    stage_b(0)
                    stage_b(1)
                    stage_c(0)
                    stage_c(1)

            @pl.when(s > 0)
            def _():
                update_phase(b)

            if b == 1:
                qall[me] = qacc[...]
                for p in range(3):
                    small_q(p).start()

                @pl.when(s == NUM_STEPS - 1)
                def _():
                    out_theta().start()

            def logits(j, carry):
                @pl.when(s == 0)
                def _():
                    if b == 0:
                        load_a(j).wait()
                idx = 2 * b + j
                if b == 1:
                    @pl.when(j == 0)
                    def _():
                        stage_d(0)

                    @pl.when(j == 1)
                    def _():
                        stage_d(1)
                zbuf[idx] = lax.dot_general(
                    tb[pl.ds(pl.multiple_of(new_rows[b], HB), HB), :],
                    a[pl.ds(pl.multiple_of(j * 512, 512), 512), :], NT, preferred_element_type=F32)
                stage_a(idx)
                return carry
            lax.fori_loop(0, 2, logits, 0)

        stage_b(2)
        nbase = 256 * par

        def gram(b, carry):
            rows = jnp.where(b == 0, 512 * par, HB)
            g = lax.dot_general(
                tb[pl.ds(pl.multiple_of(rows, HB), HB), :],
                tb[pl.ds(pl.multiple_of(nbase, HB), 512), :], NT, preferred_element_type=F32)
            zbuf[4 + b, :, pl.ds(pl.multiple_of(nbase, HB), HB)] = g[:, 0:HB]
            zbuf[4 + b, :, pl.ds(pl.multiple_of(HB - nbase, HB), HB)] = g[:, HB:]
            own = zbuf[4 + b, :, pl.ds(pl.multiple_of(b * HB, HB), HB)]
            eye = lax.broadcasted_iota(jnp.int32, (HB, HB), 0) == lax.broadcasted_iota(jnp.int32, (HB, HB), 1)
            row = jnp.sum(jnp.where(eye, own, 0.0), axis=0, keepdims=True)
            dgs[:, pl.ds(pl.multiple_of(b * HB, HB), HB)] = jnp.broadcast_to(row, (8, HB))
            stage_a(4 + b)

            @pl.when(b == 0)
            def _():
                stage_b(3)
            return carry
        lax.fori_loop(0, 2, gram, 0)
        dall[me] = dgs[...]
        for p in range(3):
            small_g(p).start()
        stage_b(4)
        stage_c(2)
        stage_e(0)
        stage_e(1)
        for p in range(3):
            small_q(p).wait_recv()
        qsum = (qall[0] + qall[1]) + (qall[2] + qall[3])
        qt[...] = jnp.concatenate([qsum, jnp.zeros((112, N), F32)], axis=0).T

        def score_phase(b):
            def body(c, carry):
                events = {(0, 1): ((stage_b, 5), (stage_c, 3), (stage_d, 2)),
                          (0, 2): ((stage_c, 4), (stage_d, 3)),
                          (0, 3): ((stage_c, 5),),
                          (1, 0): ((stage_d, 4),),
                          (1, 1): ((stage_d, 5),)}
                for (eb, ec), todo in events.items():
                    if eb == b:
                        @pl.when(c == ec)
                        def _():
                            for f, i in todo:
                                f(i)
                rr = rbuf[b * HB:(b + 1) * HB, :]
                qb = qt[b * HB:(b + 1) * HB, 0:16].astype(BF16)
                for i in range(CW // SW):
                    cs = pl.ds(pl.multiple_of(c * CW + i * SW, SW), SW)
                    lik = jnp.dot(rr, a[:, cs], preferred_element_type=F32)
                    low = jnp.dot(qb, ut_ref[:, cs], preferred_element_type=F32)
                    x = th[b * HB:(b + 1) * HB, cs] - mu_ref[:, cs]
                    sbuf[b * HB:(b + 1) * HB, cs] = (lik_weight * lik - x * lam_ref[:, cs] - low).astype(BF16)
                return carry
            lax.fori_loop(0, NC, body, 0)

        for b in range(2):
            if b == 1:
                stage_e(2)
                stage_e(3)
            score_phase(b)

            @pl.when(s == NUM_STEPS - 1)
            def _():
                out_s(b).start()
        stage_e(4)
        stage_e(5)
        for p in range(3):
            small_q(p).wait_send()
            small_g(p).wait_send()
        kx[:, 512:768] = kx[:, 0:256]
        return carry

    lax.fori_loop(0, NUM_STEPS, step, 0)
    k_copy = pltpu.make_async_copy(kx.at[:, pl.ds(0, 512)], k_out, out_sem.at[3])
    kv_copy = pltpu.make_async_copy(kv, kv_out, out_sem.at[4])
    k_copy.start()
    kv_copy.start()
    k_copy.wait()
    kv_copy.wait()
    out_theta().wait()
    out_s(0).wait()
    out_s(1).wait()


def last_kernel(consts, kb, kv, s, th, out):
    _, _, two_over_band, gain = consts
    for i in range(2):
        r = slice(i * HB, (i + 1) * HB)
        k = kb[r, :]
        t = th[...]
        drive = jnp.dot(k, s[...], preferred_element_type=F32)
        pull = jnp.dot(k, t.astype(BF16), preferred_element_type=F32)
        t = th[r, :]
        out[r, :] = t + gain * (drive + two_over_band * (kv[r, 0:1] * t - pull))


def solution(mesh):
    feat = mesh.shape["feat"]
    dim_full = D * feat
    band = 2.0 * dim_full
    consts = (2.0 / math.sqrt(M * dim_full), 1.0 / band, 2.0 / band, dim_full / 4.0 / N)

    def local_run(particles, prec_diag, low_factor, prior_mean, data_mat, labels):
        targets = labels.astype(F32)[None, :]
        vm = pl.BlockSpec(memory_space=pltpu.VMEM)
        anyspace = pl.BlockSpec(memory_space=pl.ANY)
        dma = pltpu.SemaphoreType.DMA
        th2, s2, k2, kv2 = pl.pallas_call(
            functools.partial(run_kernel, consts),
            out_shape=(jax.ShapeDtypeStruct((N, D), F32), jax.ShapeDtypeStruct((N, D), BF16),
                       jax.ShapeDtypeStruct((N, N), BF16), jax.ShapeDtypeStruct((N, 128), F32)),
            in_specs=[anyspace, vm, vm, vm, anyspace, vm],
            out_specs=(anyspace,) * 4,
            scratch_shapes=[
                pltpu.VMEM((N, D), F32), pltpu.VMEM((M, D), BF16), pltpu.VMEM((768, D), BF16),
                pltpu.VMEM((N, D), BF16),
                pltpu.VMEM((6, HB, 512), F32), pltpu.VMEM((6, 128, 512), F32), pltpu.VMEM((6, 64, 512), F32),
                pltpu.VMEM((6, 64, 512), F32), pltpu.VMEM((N, M), BF16), pltpu.VMEM((N, 768), BF16),
                pltpu.VMEM((N, 128), F32), pltpu.VMEM((16, N), F32), pltpu.VMEM((4, 16, N), F32),
                pltpu.VMEM((8, N), F32), pltpu.VMEM((4, 8, N), F32), pltpu.VMEM((N, 128), F32),
                dma((8,)), dma((2,)), dma((5,)),
                dma((6,)), dma((6,)), dma((6,)), dma((6,)), dma((6,)), dma((6,)), dma((6,)), dma((6,)),
                dma((2,)), dma((2,)), dma((2,)), dma((2,)),
                dma((3,)), dma((3,)), dma((3,)), dma((3,)),
            ],
            compiler_params=pltpu.CompilerParams(
                collective_id=0, has_side_effects=True, vmem_limit_bytes=VMEM_LIMIT),
        )(particles, prec_diag[None, :], low_factor.T, prior_mean[None, :], data_mat, targets)
        width = 1024
        return pl.pallas_call(
            functools.partial(last_kernel, consts),
            grid=(D // width,),
            out_shape=jax.ShapeDtypeStruct((N, D), F32),
            in_specs=[pl.BlockSpec((N, N), lambda i: (0, 0)), pl.BlockSpec((N, 128), lambda i: (0, 0)),
                      pl.BlockSpec((N, width), lambda i: (0, i)), pl.BlockSpec((N, width), lambda i: (0, i))],
            out_specs=pl.BlockSpec((N, width), lambda i: (0, i)),
            compiler_params=pltpu.CompilerParams(vmem_limit_bytes=48 * 2**20),
        )(k2, kv2, s2, th2)

    return jax.shard_map(
        local_run,
        mesh=mesh,
        in_specs=(P("ens", "feat"), P(("ens", "feat")), P(("ens", "feat"), None),
                  P(("ens", "feat")), P("ens", "feat"), P("ens")),
        out_specs=P("ens", "feat"),
        check_vma=False,
    )
```

```python
import functools
import math
import jax
import jax.numpy as jnp
from jax import lax
from jax.experimental import pallas as pl
from jax.experimental.pallas import tpu as pltpu
from jax.sharding import PartitionSpec as P

NUM_STEPS = 3
NT = (((1,), (1,)), ((), ()))
F32 = jnp.float32
BF16 = jnp.bfloat16
N = 512
HB = 256
D = 8192
M = 1024
CW = 2048
SW = 1024
SS = 512
NC = D // CW
VMEM_LIMIT = 67_043_328


def run_kernel(consts, th_hbm, lam_ref, ut_ref, mu_ref, a_hbm, y_ref,
               th_out, s_out, k_out, kv_out,
               th, a, tb, tn, sbuf, zbuf, ra, snd, rb, rbuf, kx, kv, qacc, qall, dall, kall, qt,
               ld_sem, a_sem, out_sem, tn_sem, as_sem, ar_sem, bs_sem, br_sem, cs_sem, cr_sem, ds_sem, dr_sem,
               qs_sem, qr_sem, gs_sem, gr_sem, ks_sem, kr_sem):
    lik_weight, inv_band, two_over_band, gain = consts
    me = lax.axis_index("feat")
    xx = me // 2
    cc = me % 2
    sib = xx * 2 + (1 - cc)
    far = (1 - xx) * 2 + cc
    diag_dev = (1 - xx) * 2 + (1 - cc)
    peers = (sib, far, diag_dev)

    def remote(src, dst, ssem, rsem, dev):
        return pltpu.make_async_remote_copy(
            src_ref=src, dst_ref=dst, send_sem=ssem, recv_sem=rsem,
            device_id={"feat": dev}, device_id_type=pl.DeviceIdType.MESH)

    def width(idx):
        return 256 if idx == 4 else 512

    def block(idx):
        return idx // 2 if idx < 4 else idx - 4

    def copy_a(idx):
        w = pl.ds(0, width(idx))
        return remote(zbuf.at[idx, pl.ds((1 - cc) * 128, 128), w], ra.at[idx, :, w],
                      as_sem.at[idx], ar_sem.at[idx], sib)

    def copy_b(idx):
        w = pl.ds(0, width(idx))
        return remote(snd.at[idx, :, w], rb.at[idx, :, w], bs_sem.at[idx], br_sem.at[idx], far)

    def region(idx, first, count):
        rows = pl.ds(block(idx) * HB + first, count)
        if idx >= 4:
            return kx.at[rows, pl.ds(0, width(idx))]
        return rbuf.at[rows, pl.ds((idx % 2) * 512, 512)]

    def copy_c(idx):
        r = region(idx, cc * 128 + xx * 64, 64)
        return remote(r, r, cs_sem.at[idx], cr_sem.at[idx], far)

    def copy_d(idx):
        r = region(idx, cc * 128, 128)
        return remote(r, r, ds_sem.at[idx], dr_sem.at[idx], sib)

    def small(buf, ssem, rsem, p):
        return remote(buf.at[me], buf.at[me], ssem.at[p], rsem.at[p], peers[p])

    small_q = functools.partial(small, qall, qs_sem, qr_sem)
    small_g = functools.partial(small, dall, gs_sem, gr_sem)
    small_k = functools.partial(small, kall, ks_sem, kr_sem)

    def stage_a(idx):
        copy_a(idx).start()

    def stage_b(idx):
        copy_a(idx).wait_recv()
        o = (1 - xx) * 64
        w = width(idx)
        snd[idx, :, 0:w] = zbuf[idx, pl.ds(cc * 128 + o, 64), 0:w] + ra[idx, pl.ds(o, 64), 0:w]
        copy_b(idx).start()

    def stage_c(idx):
        copy_b(idx).wait_recv()
        o = xx * 64
        w = width(idx)
        val = (zbuf[idx, pl.ds(cc * 128 + o, 64), 0:w] + ra[idx, pl.ds(o, 64), 0:w]) + rb[idx, :, 0:w]
        first = block(idx) * HB + cc * 128 + o
        if idx < 4:
            j = idx % 2
            res = y_ref[:, j * 512:(j + 1) * 512].astype(F32) - jax.nn.sigmoid(val)
            rbuf[pl.ds(first, 64), j * 512:(j + 1) * 512] = res.astype(BF16)
        else:
            if idx == 4:
                for p in range(3):
                    small_g(p).wait_recv()
            nj = ((dall[2 * xx] + dall[2 * xx + 1]) + (dall[2 * (1 - xx)] + dall[2 * (1 - xx) + 1]))[0:1, :]
            rid = lax.broadcasted_iota(jnp.int32, (64, N), 0) + first
            cid = lax.broadcasted_iota(jnp.int32, (64, N), 1)
            ni = jnp.sum(jnp.where(rid == cid, nj, 0.0), axis=1, keepdims=True)
            dist = jnp.maximum(ni + nj[:, 0:w] - 2.0 * val, 0.0)
            kern = jnp.exp(-dist * inv_band)
            kx[pl.ds(first, 64), 0:w] = kern.astype(BF16)
            col = jnp.sum(kern, axis=0, keepdims=True)
            if idx == 4:
                kall[me, :, 0:HB] = jnp.broadcast_to(col, (8, HB))
            else:
                kall[me, :, 0:HB] += jnp.broadcast_to(col[:, 0:HB], (8, HB))
                cross = jnp.sum(kern[:, 0:HB], axis=1, keepdims=True)
                placed = jnp.sum(jnp.where(rid[:, HB:] == cid[:, HB:], cross, 0.0), axis=0, keepdims=True)
                kall[me, :, HB:N] = jnp.broadcast_to(col[:, HB:N] + placed, (8, HB))
                for p in range(3):
                    small_k(p).start()
        copy_c(idx).start()
        copy_a(idx).wait_send()
        copy_b(idx).wait_send()

    def stage_d(idx):
        copy_c(idx).wait()
        copy_d(idx).start()

    def stage_e(idx):
        copy_d(idx).wait()

    def load_th(b, c):
        v = (pl.ds(b * HB, HB), pl.ds(pl.multiple_of(c * CW, CW), CW))
        return pltpu.make_async_copy(th_hbm.at[v], th.at[v], ld_sem.at[b * NC + c])

    def load_a(j):
        v = (pl.ds(j * 512, 512), slice(None))
        return pltpu.make_async_copy(a_hbm.at[v], a.at[v], a_sem.at[j])

    for c in range(NC):
        load_th(0, c).start()
    for j in range(2):
        load_a(j).start()
    for c in range(NC):
        load_th(1, c).start()

    barrier = pltpu.get_barrier_semaphore()
    for p in peers:
        pl.semaphore_signal(barrier, inc=1, device_id={"feat": p}, device_id_type=pl.DeviceIdType.MESH)
    pl.semaphore_wait(barrier, 3)

    def out_theta():
        return pltpu.make_async_copy(th, th_out, out_sem.at[0])

    def out_s(b):
        v = (pl.ds(b * HB, HB), slice(None))
        return pltpu.make_async_copy(sbuf.at[v], s_out.at[v], out_sem.at[1 + b])

    def keep_block0():
        return pltpu.make_async_copy(tn, tb.at[pl.ds(0, HB), :], tn_sem.at[0])

    def new_block(b):
        return tn if b == 0 else tb.at[pl.ds(HB, HB), :]

    def step(s, carry):
        def at(cond, *todo):
            @pl.when(cond)
            def _():
                for f, i in todo:
                    f(i)

        def project(b, cs, xb):
            part = lax.dot_general(ut_ref[:, cs], xb, NT, preferred_element_type=F32)
            qacc[:, b * HB:(b + 1) * HB] += part

        def load_phase(b):
            def body(c, carry):
                load_th(b, c).wait()
                for i in range(CW // SW):
                    cs = pl.ds(pl.multiple_of(c * CW + i * SW, SW), SW)
                    t = th[b * HB:(b + 1) * HB, cs]
                    new_block(b)[:, cs] = t.astype(BF16)
                    project(b, cs, (t - mu_ref[:, cs]).astype(BF16))
                return carry
            lax.fori_loop(0, NC, body, 0)

        def update_phase(b):
            def body(c, carry):
                if b == 1:
                    at(c == 1, (stage_b, 4))
                    at(c == 2, (stage_c, 0))
                kb = kx[b * HB:(b + 1) * HB, 0:N]
                kt = kx[b * HB:(b + 1) * HB, N:2 * N]
                kvb = kv[b * HB:(b + 1) * HB, 0:1]
                for i in range(CW // SW):
                    cs = pl.ds(pl.multiple_of(c * CW + i * SW, SW), SW)
                    move = (jnp.dot(kb, sbuf[:, cs], preferred_element_type=F32)
                            + jnp.dot(kt, tb[:, cs], preferred_element_type=F32))
                    t = th[b * HB:(b + 1) * HB, cs]
                    t = t + gain * (move + kvb * t)
                    th[b * HB:(b + 1) * HB, cs] = t
                    new_block(b)[:, cs] = t.astype(BF16)
                    project(b, cs, (t - mu_ref[:, cs]).astype(BF16))
                return carry
            lax.fori_loop(0, NC, body, 0)

        def logits(b, j):
            zbuf[2 * b + j] = lax.dot_general(
                new_block(b)[...], a[j * 512:(j + 1) * 512, :], NT, preferred_element_type=F32)
            stage_a(2 * b + j)

        def gram(b, cols):
            g = lax.dot_general(new_block(b)[...], new_block(cols)[...], NT, preferred_element_type=F32)
            zbuf[4 + b, :, cols * HB:(cols + 1) * HB] = g
            if cols == b:
                eye = lax.broadcasted_iota(jnp.int32, (HB, HB), 0) == lax.broadcasted_iota(jnp.int32, (HB, HB), 1)
                row = jnp.sum(jnp.where(eye, g, 0.0), axis=0, keepdims=True)
                dall[me, :, b * HB:(b + 1) * HB] = jnp.broadcast_to(row, (8, HB))

        def first_gram():
            gram(0, 0)
            stage_a(4)
            stage_b(1)

        qacc[...] = jnp.zeros_like(qacc)

        @pl.when(s == 0)
        def _():
            load_phase(0)
            load_a(0).wait()

        @pl.when(s > 0)
        def _():
            update_phase(0)

        logits(0, 0)

        @pl.when(s == 0)
        def _():
            load_a(1).wait()
        logits(0, 1)
        stage_b(0)

        @pl.when(s == 0)
        def _():
            first_gram()
            load_phase(1)
            stage_b(4)

        @pl.when(s > 0)
        def _():
            first_gram()
            update_phase(1)
            stage_c(1)

        qall[me] = qacc[...]
        for p in range(3):
            small_q(p).start()

        @pl.when(s == NUM_STEPS - 1)
        def _():
            out_theta().start()

        @pl.when(s < NUM_STEPS - 1)
        def _():
            keep_block0().start()

        logits(1, 0)
        at(s == 0, (stage_c, 0))
        at(s > 0, (stage_d, 0))
        logits(1, 1)
        at(s == 0, (stage_c, 1))
        at(s > 0, (stage_d, 1))
        stage_b(2)
        gram(1, 0)
        at(s == 0, (stage_d, 0))
        gram(1, 1)
        stage_a(5)
        for p in range(3):
            small_g(p).start()
        stage_b(3)
        at(s == 0, (stage_d, 1))
        stage_e(0)
        stage_e(1)
        for p in range(3):
            small_q(p).wait_recv()
        qsum = (qall[0] + qall[1]) + (qall[2] + qall[3])
        qt[...] = jnp.concatenate([qsum, jnp.zeros((112, N), F32)], axis=0).T

        def score_phase(b, events):
            def body(c, carry):
                for when, todo in events.items():
                    at(c == when, *todo)
                rr = rbuf[b * HB:(b + 1) * HB, :]
                qb = qt[b * HB:(b + 1) * HB, 0:16].astype(BF16)
                for i in range(CW // SS):
                    cs = pl.ds(pl.multiple_of(c * CW + i * SS, SS), SS)
                    lik = jnp.dot(rr, a[:, cs], preferred_element_type=F32)
                    low = jnp.dot(qb, ut_ref[:, cs], preferred_element_type=F32)
                    x = th[b * HB:(b + 1) * HB, cs] - mu_ref[:, cs]
                    sbuf[b * HB:(b + 1) * HB, cs] = (lik_weight * lik - x * lam_ref[:, cs] - low).astype(BF16)
                return carry
            lax.fori_loop(0, NC, body, 0)

            @pl.when(s == NUM_STEPS - 1)
            def _():
                out_s(b).start()

        score_phase(0, {1: [(stage_c, 2)], 2: [(stage_c, 4)], 3: [(stage_c, 3), (stage_b, 5)]})
        for idx in (2, 3, 4):
            stage_d(idx)
        stage_e(2)
        stage_e(3)
        score_phase(1, {2: [(stage_c, 5)]})
        stage_e(4)
        stage_d(5)
        for p in range(3):
            small_k(p).wait_recv()
        ksum = (kall[0] + kall[1]) + (kall[2] + kall[3])
        kv[...] = jnp.broadcast_to(two_over_band * ksum[0:1, :], (128, N)).T
        stage_e(5)
        kx[0:HB, HB:N] = kx[HB:N, 0:HB].astype(F32).T.astype(BF16)
        kx[:, N:2 * N] = (kx[:, 0:N].astype(F32) * -two_over_band).astype(BF16)
        for p in range(3):
            small_q(p).wait_send()
            small_g(p).wait_send()
            small_k(p).wait_send()

        @pl.when(s < NUM_STEPS - 1)
        def _():
            keep_block0().wait()
        return carry

    lax.fori_loop(0, NUM_STEPS, step, 0)
    k_copy = pltpu.make_async_copy(kx, k_out, out_sem.at[3])
    kv_copy = pltpu.make_async_copy(kv, kv_out, out_sem.at[4])
    k_copy.start()
    kv_copy.start()
    k_copy.wait()
    kv_copy.wait()
    out_theta().wait()
    out_s(0).wait()
    out_s(1).wait()


def last_kernel(gain, kx, kv, s, th, out):
    for i in range(s.shape[1] // 512):
        cs = slice(i * 512, (i + 1) * 512)
        t = th[:, cs]
        move = (jnp.dot(kx[:, 0:N], s[:, cs], preferred_element_type=F32)
                + jnp.dot(kx[:, N:2 * N], t.astype(BF16), preferred_element_type=F32))
        out[:, cs] = t + gain * (move + kv[:, 0:1] * t)


def solution(mesh):
    feat = mesh.shape["feat"]
    dim_full = D * feat
    band = 2.0 * dim_full
    consts = (2.0 / math.sqrt(M * dim_full), 1.0 / band, 2.0 / band, dim_full / 4.0 / N)

    def local_run(particles, prec_diag, low_factor, prior_mean, data_mat, labels):
        targets = labels[None, :]
        vm = pl.BlockSpec(memory_space=pltpu.VMEM)
        anyspace = pl.BlockSpec(memory_space=pl.ANY)
        dma = pltpu.SemaphoreType.DMA
        th2, s2, k2, kv2 = pl.pallas_call(
            functools.partial(run_kernel, consts),
            out_shape=(jax.ShapeDtypeStruct((N, D), F32), jax.ShapeDtypeStruct((N, D), BF16),
                       jax.ShapeDtypeStruct((N, 2 * N), BF16), jax.ShapeDtypeStruct((N, 128), F32)),
            in_specs=[anyspace, vm, vm, vm, anyspace, vm],
            out_specs=(anyspace,) * 4,
            scratch_shapes=[
                pltpu.VMEM((N, D), F32), pltpu.VMEM((M, D), BF16), pltpu.VMEM((N, D), BF16), pltpu.VMEM((HB, D), BF16),
                pltpu.VMEM((N, D), BF16),
                pltpu.VMEM((6, HB, 512), F32), pltpu.VMEM((6, 128, 512), F32), pltpu.VMEM((6, 64, 512), F32),
                pltpu.VMEM((6, 64, 512), F32), pltpu.VMEM((N, M), BF16), pltpu.VMEM((N, 2 * N), BF16),
                pltpu.VMEM((N, 128), F32), pltpu.VMEM((16, N), F32), pltpu.VMEM((4, 16, N), F32),
                pltpu.VMEM((4, 8, N), F32), pltpu.VMEM((4, 8, N), F32), pltpu.VMEM((N, 128), F32),
                dma((8,)), dma((2,)), dma((5,)), dma((1,)),
                dma((6,)), dma((6,)), dma((6,)), dma((6,)), dma((6,)), dma((6,)), dma((6,)), dma((6,)),
                dma((3,)), dma((3,)), dma((3,)), dma((3,)), dma((3,)), dma((3,)),
            ],
            compiler_params=pltpu.CompilerParams(
                collective_id=0, has_side_effects=True, vmem_limit_bytes=VMEM_LIMIT),
        )(particles, prec_diag[None, :], low_factor.T, prior_mean[None, :], data_mat, targets)
        width = 1024
        return pl.pallas_call(
            functools.partial(last_kernel, consts[3]),
            grid=(D // width,),
            out_shape=jax.ShapeDtypeStruct((N, D), F32),
            in_specs=[pl.BlockSpec((N, 2 * N), lambda i: (0, 0)), pl.BlockSpec((N, 128), lambda i: (0, 0)),
                      pl.BlockSpec((N, width), lambda i: (0, i)), pl.BlockSpec((N, width), lambda i: (0, i))],
            out_specs=pl.BlockSpec((N, width), lambda i: (0, i)),
            compiler_params=pltpu.CompilerParams(vmem_limit_bytes=VMEM_LIMIT),
        )(k2, kv2, s2, th2)

    return jax.shard_map(
        local_run,
        mesh=mesh,
        in_specs=(P("ens", "feat"), P(("ens", "feat")), P(("ens", "feat"), None),
                  P(("ens", "feat")), P("ens", "feat"), P("ens")),
        out_specs=P("ens", "feat"),
        check_vma=False,
    )
```

```python
import functools
import math
import jax
import jax.numpy as jnp
from jax import lax
from jax.experimental import pallas as pl
from jax.experimental.pallas import tpu as pltpu
from jax.sharding import PartitionSpec as P

NUM_STEPS = 3
NT = (((1,), (1,)), ((), ()))
F32 = jnp.float32
BF16 = jnp.bfloat16
N = 512
HB = 256
D = 8192
M = 1024
CW = 2048
SW = 1024
SS = 512
NC = D // CW
LW = 1024
AHEAD = 4
VMEM_LIMIT = 67_043_328


def run_kernel(consts, th_hbm, lam_ref, ut_ref, mu_ref, a_hbm, y_ref,
               th_out, s_out, k_out, kv_out,
               th, a, tb, tn, sbuf, zbuf, ra, snd, rb, rbuf, kx, kv, qacc, qall, dall, kall, qt,
               ld_sem, a_sem, out_sem, tn_sem, as_sem, ar_sem, bs_sem, br_sem, cs_sem, cr_sem, ds_sem, dr_sem,
               qs_sem, qr_sem, gs_sem, gr_sem, ks_sem, kr_sem):
    lik_weight, inv_band, two_over_band, gain = consts
    me = lax.axis_index("feat")
    xx = me // 2
    cc = me % 2
    sib = xx * 2 + (1 - cc)
    far = (1 - xx) * 2 + cc
    diag_dev = (1 - xx) * 2 + (1 - cc)
    peers = (sib, far, diag_dev)

    def remote(src, dst, ssem, rsem, dev):
        return pltpu.make_async_remote_copy(
            src_ref=src, dst_ref=dst, send_sem=ssem, recv_sem=rsem,
            device_id={"feat": dev}, device_id_type=pl.DeviceIdType.MESH)

    def width(idx):
        return 256 if idx == 4 else 512

    def block(idx):
        return idx // 2 if idx < 4 else idx - 4

    def copy_a(idx):
        w = pl.ds(0, width(idx))
        return remote(zbuf.at[idx, pl.ds((1 - cc) * 128, 128), w], ra.at[idx, :, w],
                      as_sem.at[idx], ar_sem.at[idx], sib)

    def copy_b(idx):
        w = pl.ds(0, width(idx))
        return remote(snd.at[idx, :, w], rb.at[idx, :, w], bs_sem.at[idx], br_sem.at[idx], far)

    def region(idx, first, count):
        rows = pl.ds(block(idx) * HB + first, count)
        if idx >= 4:
            return kx.at[rows, pl.ds(0, width(idx))]
        return rbuf.at[rows, pl.ds((idx % 2) * 512, 512)]

    def copy_c(idx):
        r = region(idx, cc * 128 + xx * 64, 64)
        return remote(r, r, cs_sem.at[idx], cr_sem.at[idx], far)

    def copy_d(idx):
        r = region(idx, cc * 128, 128)
        return remote(r, r, ds_sem.at[idx], dr_sem.at[idx], sib)

    def small(buf, ssem, rsem, p):
        return remote(buf.at[me], buf.at[me], ssem.at[p], rsem.at[p], peers[p])

    small_q = functools.partial(small, qall, qs_sem, qr_sem)
    small_g = functools.partial(small, dall, gs_sem, gr_sem)
    small_k = functools.partial(small, kall, ks_sem, kr_sem)

    def stage_a(idx):
        copy_a(idx).start()

    def stage_b(idx):
        copy_a(idx).wait_recv()
        o = (1 - xx) * 64
        w = width(idx)
        snd[idx, :, 0:w] = zbuf[idx, pl.ds(cc * 128 + o, 64), 0:w] + ra[idx, pl.ds(o, 64), 0:w]
        copy_b(idx).start()

    def stage_c(idx):
        copy_b(idx).wait_recv()
        o = xx * 64
        w = width(idx)
        val = (zbuf[idx, pl.ds(cc * 128 + o, 64), 0:w] + ra[idx, pl.ds(o, 64), 0:w]) + rb[idx, :, 0:w]
        first = block(idx) * HB + cc * 128 + o
        if idx < 4:
            j = idx % 2
            res = y_ref[:, j * 512:(j + 1) * 512].astype(F32) - jax.nn.sigmoid(val)
            rbuf[pl.ds(first, 64), j * 512:(j + 1) * 512] = res.astype(BF16)
        else:
            if idx == 5:
                for p in range(3):
                    small_g(p).wait_recv()
            nj = ((dall[2 * xx] + dall[2 * xx + 1]) + (dall[2 * (1 - xx)] + dall[2 * (1 - xx) + 1]))[0:1, :]
            rid = lax.broadcasted_iota(jnp.int32, (64, N), 0) + first
            cid = lax.broadcasted_iota(jnp.int32, (64, N), 1)
            ni = jnp.sum(jnp.where(rid == cid, nj, 0.0), axis=1, keepdims=True)
            dist = jnp.maximum(ni + nj[:, 0:w] - 2.0 * val, 0.0)
            kern = jnp.exp(-dist * inv_band)
            kx[pl.ds(first, 64), 0:w] = kern.astype(BF16)
            col = jnp.sum(kern, axis=0, keepdims=True)
            if idx == 4:
                kall[me, :, 0:HB] += jnp.broadcast_to(col, (8, HB))
                for p in range(3):
                    small_k(p).start()
            else:
                kall[me, :, 0:HB] = jnp.broadcast_to(col[:, 0:HB], (8, HB))
                cross = jnp.sum(kern[:, 0:HB], axis=1, keepdims=True)
                placed = jnp.sum(jnp.where(rid[:, HB:] == cid[:, HB:], cross, 0.0), axis=0, keepdims=True)
                kall[me, :, HB:N] = jnp.broadcast_to(col[:, HB:N] + placed, (8, HB))
        copy_c(idx).start()
        copy_a(idx).wait_send()
        copy_b(idx).wait_send()

    def stage_d(idx):
        copy_c(idx).wait()
        copy_d(idx).start()

    def stage_e(idx):
        copy_d(idx).wait()

    def load_th(b, c):
        v = (pl.ds(b * HB, HB), pl.ds(pl.multiple_of(c * CW, CW), CW))
        return pltpu.make_async_copy(th_hbm.at[v], th.at[v], ld_sem.at[b * NC + c])

    def load_a(j, c):
        v = (pl.ds(j * 512 + c * 128, 128), slice(None))
        return pltpu.make_async_copy(a_hbm.at[v], a.at[v], a_sem.at[j * 4 + c])

    for c in range(NC):
        load_th(0, c).start()

    barrier = pltpu.get_barrier_semaphore()
    for p in peers:
        pl.semaphore_signal(barrier, inc=1, device_id={"feat": p}, device_id_type=pl.DeviceIdType.MESH)
    pl.semaphore_wait(barrier, 3)

    def out_theta():
        return pltpu.make_async_copy(th, th_out, out_sem.at[0])

    def out_s(b):
        v = (pl.ds(b * HB, HB), slice(None))
        return pltpu.make_async_copy(sbuf.at[v], s_out.at[v], out_sem.at[1 + b])

    def keep_block0():
        return pltpu.make_async_copy(tn, tb.at[pl.ds(0, HB), :], tn_sem.at[0])

    def new_block(b):
        return tn if b == 0 else tb.at[pl.ds(HB, HB), :]

    def step(s, carry):
        def at(cond, *todo):
            @pl.when(cond)
            def _():
                for f, i in todo:
                    f(i)

        def project():
            def body(c, carry):
                at(c == 2, (stage_b, 3))
                cs = pl.ds(pl.multiple_of(c * CW, CW), CW)
                xb = (th[:, cs] - mu_ref[:, cs]).astype(BF16)
                qacc[...] += lax.dot_general(ut_ref[:, cs], xb, NT, preferred_element_type=F32)
                return carry
            qacc[...] = jnp.zeros_like(qacc)
            lax.fori_loop(0, NC, body, 0)

        def load_phase(b):
            def body(c, carry):
                load_th(b, c).wait()
                if b == 0:
                    load_a(0, c).start()
                for i in range(CW // SW):
                    cs = pl.ds(pl.multiple_of(c * CW + i * SW, SW), SW)
                    t = th[b * HB:(b + 1) * HB, cs]
                    new_block(b)[:, cs] = t.astype(BF16)
                return carry
            lax.fori_loop(0, NC, body, 0)

        def update_phase(b):
            def body(c, carry):
                if b == 1:
                    at(c == 1, (stage_b, 1))
                    at(c == 3, (stage_c, 0))
                kb = kx[b * HB:(b + 1) * HB, 0:N]
                kt = kx[b * HB:(b + 1) * HB, N:2 * N]
                kvb = kv[b * HB:(b + 1) * HB, 0:1]
                for i in range(CW // SW):
                    cs = pl.ds(pl.multiple_of(c * CW + i * SW, SW), SW)
                    move = (jnp.dot(kb, sbuf[:, cs], preferred_element_type=F32)
                            + jnp.dot(kt, tb[:, cs], preferred_element_type=F32))
                    t = th[b * HB:(b + 1) * HB, cs]
                    t = t + gain * (move + kvb * t)
                    th[b * HB:(b + 1) * HB, cs] = t
                    new_block(b)[:, cs] = t.astype(BF16)
                return carry
            lax.fori_loop(0, NC, body, 0)

        def logits(b, j):
            zbuf[2 * b + j] = lax.dot_general(
                new_block(b)[...], a[j * 512:(j + 1) * 512, :], NT, preferred_element_type=F32)
            stage_a(2 * b + j)

        def gram(b, cols):
            g = lax.dot_general(new_block(b)[...], new_block(cols)[...], NT, preferred_element_type=F32)
            zbuf[4 + b, :, cols * HB:(cols + 1) * HB] = g
            if cols == b:
                eye = lax.broadcasted_iota(jnp.int32, (HB, HB), 0) == lax.broadcasted_iota(jnp.int32, (HB, HB), 1)
                row = jnp.sum(jnp.where(eye, g, 0.0), axis=0, keepdims=True)
                dall[me, :, b * HB:(b + 1) * HB] = jnp.broadcast_to(row, (8, HB))

        @pl.when(s == 0)
        def _():
            load_phase(0)
            for c in range(4):
                load_a(0, c).wait()
                load_a(1, c).start()

        @pl.when(s > 0)
        def _():
            update_phase(0)

        logits(0, 0)

        @pl.when(s == 0)
        def _():
            for c in range(4):
                load_a(1, c).wait()
                load_th(1, c).start()
        logits(0, 1)
        stage_b(0)

        @pl.when(s == 0)
        def _():
            load_phase(1)
            stage_b(1)

        @pl.when(s > 0)
        def _():
            update_phase(1)

        @pl.when(s == NUM_STEPS - 1)
        def _():
            out_theta().start()

        @pl.when(s < NUM_STEPS - 1)
        def _():
            keep_block0().start()

        logits(1, 0)
        at(s == 0, (stage_c, 0))
        at(s > 0, (stage_c, 1), (stage_d, 0))
        logits(1, 1)
        at(s == 0, (stage_c, 1))
        stage_b(2)
        project()
        qall[me] = qacc[...]
        for p in range(3):
            small_q(p).start()
        gram(1, 0)
        at(s == 0, (stage_d, 0))
        at(s > 0, (stage_d, 1))
        gram(1, 1)
        stage_a(5)
        stage_c(2)
        at(s == 0, (stage_d, 1))
        gram(0, 0)
        stage_a(4)
        for p in range(3):
            small_g(p).start()
        stage_e(0)
        stage_e(1)
        for p in range(3):
            small_q(p).wait_recv()
        qsum = (qall[0] + qall[1]) + (qall[2] + qall[3])
        qt[...] = jnp.concatenate([qsum, jnp.zeros((112, N), F32)], axis=0).T

        def score_phase(b, events):
            def body(c, carry):
                for when, todo in events.items():
                    at(c == when, *todo)
                rr = rbuf[b * HB:(b + 1) * HB, :]
                qb = qt[b * HB:(b + 1) * HB, 0:16].astype(BF16)
                for i in range(CW // SS):
                    cs = pl.ds(pl.multiple_of(c * CW + i * SS, SS), SS)
                    lik = jnp.dot(rr, a[:, cs], preferred_element_type=F32)
                    low = jnp.dot(qb, ut_ref[:, cs], preferred_element_type=F32)
                    x = th[b * HB:(b + 1) * HB, cs] - mu_ref[:, cs]
                    sbuf[b * HB:(b + 1) * HB, cs] = (lik_weight * lik - x * lam_ref[:, cs] - low).astype(BF16)
                return carry
            lax.fori_loop(0, NC, body, 0)

            @pl.when(s == NUM_STEPS - 1)
            def _():
                out_s(b).start()

        score_phase(0, {1: [(stage_c, 3)], 2: [(stage_d, 2), (stage_b, 5)], 3: [(stage_b, 4), (stage_d, 3)]})
        stage_e(2)
        stage_e(3)
        score_phase(1, {1: [(stage_c, 5)], 2: [(stage_c, 4)]})
        stage_d(5)
        stage_d(4)
        stage_e(4)
        for p in range(3):
            small_k(p).wait_recv()
        ksum = (kall[0] + kall[1]) + (kall[2] + kall[3])
        kv[...] = jnp.broadcast_to(two_over_band * ksum[0:1, :], (128, N)).T
        stage_e(5)
        kx[0:HB, HB:N] = kx[HB:N, 0:HB].astype(F32).T.astype(BF16)
        kx[:, N:2 * N] = (kx[:, 0:N].astype(F32) * -two_over_band).astype(BF16)
        for p in range(3):
            small_q(p).wait_send()
            small_g(p).wait_send()
            small_k(p).wait_send()

        @pl.when(s < NUM_STEPS - 1)
        def _():
            keep_block0().wait()
        return carry

    lax.fori_loop(0, NUM_STEPS, step, 0)
    k_copy = pltpu.make_async_copy(kx, k_out, out_sem.at[3])
    kv_copy = pltpu.make_async_copy(kv, kv_out, out_sem.at[4])
    k_copy.start()
    kv_copy.start()
    k_copy.wait()
    kv_copy.wait()
    out_theta().wait()
    out_s(0).wait()
    out_s(1).wait()


def last_kernel(gain, kx_hbm, kv_hbm, s_hbm, th_hbm, out_hbm, kx, kv, s, th, k_sem, s_sem, th_sem, out_sem):
    blocks = D // LW

    def copy(src, dst, sem, c):
        cs = pl.ds(pl.multiple_of(c * LW, LW), LW)
        return pltpu.make_async_copy(src.at[:, cs], dst.at[:, cs], sem.at[c])

    def fetch(c):
        copy(s_hbm, s, s_sem, c).start()
        copy(th_hbm, th, th_sem, c).start()

    k_copy = pltpu.make_async_copy(kx_hbm, kx, k_sem.at[0])
    kv_copy = pltpu.make_async_copy(kv_hbm, kv, k_sem.at[1])
    k_copy.start()
    kv_copy.start()
    for c in range(AHEAD):
        fetch(c)
    k_copy.wait()
    kv_copy.wait()

    def body(c, carry):
        copy(s_hbm, s, s_sem, c).wait()
        copy(th_hbm, th, th_sem, c).wait()

        @pl.when(c + AHEAD < blocks)
        def _():
            fetch(c + AHEAD)
        cs = pl.ds(pl.multiple_of(c * LW, LW), LW)
        t = th[:, cs]
        move = (jnp.dot(kx[:, 0:N], s[:, cs], preferred_element_type=F32)
                + jnp.dot(kx[:, N:2 * N], t.astype(BF16), preferred_element_type=F32))
        th[:, cs] = t + gain * (move + kv[:, 0:1] * t)
        copy(th, out_hbm, out_sem, c).start()
        return carry
    lax.fori_loop(0, blocks, body, 0)

    def drain(c, carry):
        copy(th, out_hbm, out_sem, c).wait()
        return carry
    lax.fori_loop(0, blocks, drain, 0)


def solution(mesh):
    feat = mesh.shape["feat"]
    dim_full = D * feat
    band = 2.0 * dim_full
    consts = (2.0 / math.sqrt(M * dim_full), 1.0 / band, 2.0 / band, dim_full / 4.0 / N)

    def local_run(particles, prec_diag, low_factor, prior_mean, data_mat, labels):
        targets = labels[None, :]
        vm = pl.BlockSpec(memory_space=pltpu.VMEM)
        anyspace = pl.BlockSpec(memory_space=pl.ANY)
        dma = pltpu.SemaphoreType.DMA
        th2, s2, k2, kv2 = pl.pallas_call(
            functools.partial(run_kernel, consts),
            out_shape=(jax.ShapeDtypeStruct((N, D), F32), jax.ShapeDtypeStruct((N, D), BF16),
                       jax.ShapeDtypeStruct((N, 2 * N), BF16), jax.ShapeDtypeStruct((N, 128), F32)),
            in_specs=[anyspace, vm, vm, vm, anyspace, vm],
            out_specs=(anyspace,) * 4,
            scratch_shapes=[
                pltpu.VMEM((N, D), F32), pltpu.VMEM((M, D), BF16), pltpu.VMEM((N, D), BF16), pltpu.VMEM((HB, D), BF16),
                pltpu.VMEM((N, D), BF16),
                pltpu.VMEM((6, HB, 512), F32), pltpu.VMEM((6, 128, 512), F32), pltpu.VMEM((6, 64, 512), F32),
                pltpu.VMEM((6, 64, 512), F32), pltpu.VMEM((N, M), BF16), pltpu.VMEM((N, 2 * N), BF16),
                pltpu.VMEM((N, 128), F32), pltpu.VMEM((16, N), F32), pltpu.VMEM((4, 16, N), F32),
                pltpu.VMEM((4, 8, N), F32), pltpu.VMEM((4, 8, N), F32), pltpu.VMEM((N, 128), F32),
                dma((8,)), dma((8,)), dma((5,)), dma((1,)),
                dma((6,)), dma((6,)), dma((6,)), dma((6,)), dma((6,)), dma((6,)), dma((6,)), dma((6,)),
                dma((3,)), dma((3,)), dma((3,)), dma((3,)), dma((3,)), dma((3,)),
            ],
            compiler_params=pltpu.CompilerParams(
                collective_id=0, has_side_effects=True, vmem_limit_bytes=VMEM_LIMIT),
        )(particles, prec_diag[None, :], low_factor.T, prior_mean[None, :], data_mat, targets)
        return pl.pallas_call(
            functools.partial(last_kernel, consts[3]),
            out_shape=jax.ShapeDtypeStruct((N, D), F32),
            in_specs=[anyspace] * 4,
            out_specs=anyspace,
            scratch_shapes=[
                pltpu.VMEM((N, 2 * N), BF16), pltpu.VMEM((N, 128), F32), pltpu.VMEM((N, D), BF16), pltpu.VMEM((N, D), F32),
                dma((2,)), dma((D // LW,)), dma((D // LW,)), dma((D // LW,)),
            ],
            compiler_params=pltpu.CompilerParams(vmem_limit_bytes=VMEM_LIMIT),
        )(k2, kv2, s2, th2)

    return jax.shard_map(
        local_run,
        mesh=mesh,
        in_specs=(P("ens", "feat"), P(("ens", "feat")), P(("ens", "feat"), None),
                  P(("ens", "feat")), P("ens", "feat"), P("ens")),
        out_specs=P("ens", "feat"),
        check_vma=False,
    )
```

```python
import functools
import math
import jax
import jax.numpy as jnp
from jax import lax
from jax.experimental import pallas as pl
from jax.experimental.pallas import tpu as pltpu
from jax.sharding import PartitionSpec as P

NUM_STEPS = 3
NT = (((1,), (1,)), ((), ()))
F32 = jnp.float32
BF16 = jnp.bfloat16
N = 512
HB = 256
D = 8192
M = 1024
CW = 2048
SW = 1024
SS = 512
NC = D // CW
LW = 1024
AHEAD = 4
VMEM_LIMIT = 67_043_328


def run_kernel(consts, th_hbm, lam_ref, ut_ref, mu_ref, a_hbm, y_ref,
               th_out, s_out, k_out, kv_out,
               th, a, tb, tn, sbuf, zbuf, ra, snd, rb, rbuf, kx, kv, qacc, qall, dall, kall, qt,
               ld_sem, a_sem, out_sem, tn_sem, as_sem, ar_sem, bs_sem, br_sem, cs_sem, cr_sem, ds_sem, dr_sem,
               qs_sem, qr_sem, gs_sem, gr_sem, ks_sem, kr_sem):
    lik_weight, inv_band, two_over_band, gain = consts
    me = lax.axis_index("feat")
    xx = me // 2
    cc = me % 2
    sib = xx * 2 + (1 - cc)
    far = (1 - xx) * 2 + cc
    diag_dev = (1 - xx) * 2 + (1 - cc)
    peers = (sib, far, diag_dev)

    def remote(src, dst, ssem, rsem, dev):
        return pltpu.make_async_remote_copy(
            src_ref=src, dst_ref=dst, send_sem=ssem, recv_sem=rsem,
            device_id={"feat": dev}, device_id_type=pl.DeviceIdType.MESH)

    def width(idx):
        return 256 if idx == 4 else 512

    def block(idx):
        return idx // 2 if idx < 4 else idx - 4

    def copy_a(idx):
        w = pl.ds(0, width(idx))
        return remote(zbuf.at[idx, pl.ds((1 - cc) * 128, 128), w], ra.at[idx, :, w],
                      as_sem.at[idx], ar_sem.at[idx], sib)

    def copy_b(idx):
        w = pl.ds(0, width(idx))
        return remote(snd.at[idx, :, w], rb.at[idx, :, w], bs_sem.at[idx], br_sem.at[idx], far)

    def region(idx, first, count):
        rows = pl.ds(block(idx) * HB + first, count)
        if idx >= 4:
            return kx.at[rows, pl.ds(0, width(idx))]
        return rbuf.at[rows, pl.ds((idx % 2) * 512, 512)]

    def copy_c(idx):
        r = region(idx, cc * 128 + xx * 64, 64)
        return remote(r, r, cs_sem.at[idx], cr_sem.at[idx], far)

    def copy_d(idx):
        r = region(idx, cc * 128, 128)
        return remote(r, r, ds_sem.at[idx], dr_sem.at[idx], sib)

    def small(buf, ssem, rsem, p):
        return remote(buf.at[me], buf.at[me], ssem.at[p], rsem.at[p], peers[p])

    small_q = functools.partial(small, qall, qs_sem, qr_sem)
    small_g = functools.partial(small, dall, gs_sem, gr_sem)
    small_k = functools.partial(small, kall, ks_sem, kr_sem)

    def stage_a(idx):
        copy_a(idx).start()

    def stage_b(idx):
        copy_a(idx).wait_recv()
        o = (1 - xx) * 64
        w = width(idx)
        snd[idx, :, 0:w] = zbuf[idx, pl.ds(cc * 128 + o, 64), 0:w] + ra[idx, pl.ds(o, 64), 0:w]
        copy_b(idx).start()

    def stage_c(idx):
        copy_b(idx).wait_recv()
        o = xx * 64
        w = width(idx)
        val = (zbuf[idx, pl.ds(cc * 128 + o, 64), 0:w] + ra[idx, pl.ds(o, 64), 0:w]) + rb[idx, :, 0:w]
        first = block(idx) * HB + cc * 128 + o
        if idx < 4:
            j = idx % 2
            res = y_ref[:, j * 512:(j + 1) * 512].astype(F32) - jax.nn.sigmoid(val)
            rbuf[pl.ds(first, 64), j * 512:(j + 1) * 512] = res.astype(BF16)
        else:
            if idx == 5:
                for p in range(3):
                    small_g(p).wait_recv()
            nj = ((dall[2 * xx] + dall[2 * xx + 1]) + (dall[2 * (1 - xx)] + dall[2 * (1 - xx) + 1]))[0:1, :]
            rid = lax.broadcasted_iota(jnp.int32, (64, N), 0) + first
            cid = lax.broadcasted_iota(jnp.int32, (64, N), 1)
            ni = jnp.sum(jnp.where(rid == cid, nj, 0.0), axis=1, keepdims=True)
            dist = jnp.maximum(ni + nj[:, 0:w] - 2.0 * val, 0.0)
            kern = jnp.exp(-dist * inv_band)
            kx[pl.ds(first, 64), 0:w] = kern.astype(BF16)
            col = jnp.sum(kern, axis=0, keepdims=True)
            if idx == 4:
                kall[me, :, 0:HB] += jnp.broadcast_to(col, (8, HB))
                for p in range(3):
                    small_k(p).start()
            else:
                kall[me, :, 0:HB] = jnp.broadcast_to(col[:, 0:HB], (8, HB))
                cross = jnp.sum(kern[:, 0:HB], axis=1, keepdims=True)
                placed = jnp.sum(jnp.where(rid[:, HB:] == cid[:, HB:], cross, 0.0), axis=0, keepdims=True)
                kall[me, :, HB:N] = jnp.broadcast_to(col[:, HB:N] + placed, (8, HB))
        copy_c(idx).start()
        copy_a(idx).wait_send()
        copy_b(idx).wait_send()

    def stage_d(idx):
        copy_c(idx).wait()
        copy_d(idx).start()

    def stage_e(idx):
        copy_d(idx).wait()

    def load_th(b, c):
        v = (pl.ds(b * HB, HB), pl.ds(pl.multiple_of(c * CW, CW), CW))
        return pltpu.make_async_copy(th_hbm.at[v], th.at[v], ld_sem.at[b * NC + c])

    def load_a(j, c):
        v = (pl.ds(j * 512 + c * 128, 128), slice(None))
        return pltpu.make_async_copy(a_hbm.at[v], a.at[v], a_sem.at[j * 4 + c])

    for c in range(NC):
        load_th(0, c).start()

    barrier = pltpu.get_barrier_semaphore()
    for p in peers:
        pl.semaphore_signal(barrier, inc=1, device_id={"feat": p}, device_id_type=pl.DeviceIdType.MESH)
    pl.semaphore_wait(barrier, 3)

    def out_theta():
        return pltpu.make_async_copy(th, th_out, out_sem.at[0])

    def out_s(b):
        v = (pl.ds(b * HB, HB), slice(None))
        return pltpu.make_async_copy(sbuf.at[v], s_out.at[v], out_sem.at[1 + b])

    def keep_block0():
        return pltpu.make_async_copy(tn, tb.at[pl.ds(0, HB), :], tn_sem.at[0])

    def new_block(b):
        return tn if b == 0 else tb.at[pl.ds(HB, HB), :]

    def step(s, carry):
        def at(cond, *todo):
            @pl.when(cond)
            def _():
                for f, i in todo:
                    f(i)

        def project():
            def body(c, carry):
                at(c == 2, (stage_b, 3))
                cs = pl.ds(pl.multiple_of(c * CW, CW), CW)
                xb = (th[:, cs] - mu_ref[:, cs]).astype(BF16)
                qacc[...] += lax.dot_general(ut_ref[:, cs], xb, NT, preferred_element_type=F32)
                return carry
            qacc[...] = jnp.zeros_like(qacc)
            lax.fori_loop(0, NC, body, 0)

        def load_phase(b):
            def body(c, carry):
                load_th(b, c).wait()
                if b == 0:
                    load_a(0, c).start()
                for i in range(CW // SW):
                    cs = pl.ds(pl.multiple_of(c * CW + i * SW, SW), SW)
                    t = th[b * HB:(b + 1) * HB, cs]
                    new_block(b)[:, cs] = t.astype(BF16)
                return carry
            lax.fori_loop(0, NC, body, 0)

        def update_phase(b, cw):
            def body(c, carry):
                if b == 1:
                    at(c == 1, (stage_b, 1))
                    at(c == 3, (stage_c, 0))
                kb = kx[b * HB:(b + 1) * HB, 0:N]
                kt = kx[b * HB:(b + 1) * HB, N:2 * N]
                kvb = kv[b * HB:(b + 1) * HB, 0:1]
                for i in range(cw // SW):
                    cs = pl.ds(pl.multiple_of(c * cw + i * SW, SW), SW)
                    move = (jnp.dot(kb, sbuf[:, cs], preferred_element_type=F32)
                            + jnp.dot(kt, tb[:, cs], preferred_element_type=F32))
                    t = th[b * HB:(b + 1) * HB, cs]
                    t = t + gain * (move + kvb * t)
                    th[b * HB:(b + 1) * HB, cs] = t
                    new_block(b)[:, cs] = t.astype(BF16)
                return carry
            lax.fori_loop(0, D // cw, body, 0)

        def logits(b, j):
            zbuf[2 * b + j] = lax.dot_general(
                new_block(b)[...], a[j * 512:(j + 1) * 512, :], NT, preferred_element_type=F32)
            stage_a(2 * b + j)

        def gram(b, cols):
            g = lax.dot_general(new_block(b)[...], new_block(cols)[...], NT, preferred_element_type=F32)
            zbuf[4 + b, :, cols * HB:(cols + 1) * HB] = g
            if cols == b:
                eye = lax.broadcasted_iota(jnp.int32, (HB, HB), 0) == lax.broadcasted_iota(jnp.int32, (HB, HB), 1)
                row = jnp.sum(jnp.where(eye, g, 0.0), axis=0, keepdims=True)
                dall[me, :, b * HB:(b + 1) * HB] = jnp.broadcast_to(row, (8, HB))

        @pl.when(s == 0)
        def _():
            load_phase(0)
            gram(0, 0)
            for c in range(4):
                load_a(0, c).wait()
                load_a(1, c).start()

        @pl.when(s > 0)
        def _():
            update_phase(0, 4096)

        logits(0, 0)

        @pl.when(s == 0)
        def _():
            for c in range(4):
                load_a(1, c).wait()
                load_th(1, c).start()
        logits(0, 1)
        stage_b(0)

        @pl.when(s == 0)
        def _():
            load_phase(1)
            stage_b(1)

        @pl.when(s > 0)
        def _():
            update_phase(1, 2048)

        @pl.when(s == NUM_STEPS - 1)
        def _():
            out_theta().start()

        @pl.when(s < NUM_STEPS - 1)
        def _():
            keep_block0().start()

        logits(1, 0)
        at(s == 0, (stage_c, 0))
        at(s > 0, (stage_c, 1), (stage_d, 0))
        logits(1, 1)
        at(s == 0, (stage_c, 1))
        stage_b(2)
        project()
        qall[me] = qacc[...]
        for p in range(3):
            small_q(p).start()
        gram(1, 0)
        at(s == 0, (stage_d, 0))
        at(s > 0, (stage_d, 1))
        gram(1, 1)
        stage_a(5)
        stage_c(2)
        at(s == 0, (stage_d, 1))

        @pl.when(s > 0)
        def _():
            gram(0, 0)
        stage_a(4)
        for p in range(3):
            small_g(p).start()
        stage_e(0)
        stage_e(1)
        for p in range(3):
            small_q(p).wait_recv()
        qsum = (qall[0] + qall[1]) + (qall[2] + qall[3])
        qt[...] = jnp.concatenate([qsum, jnp.zeros((112, N), F32)], axis=0).T

        def score_phase(b, events):
            rr = rbuf.at[pl.ds(b * HB, HB), :]
            qb = qt.at[pl.ds(b * HB, HB), pl.ds(0, 128)]
            for i in range(D // SS):
                for f, idx in events.get(i, ()):
                    f(idx)
                cs = slice(i * SS, (i + 1) * SS)
                lik = jnp.dot(rr[...], a[:, cs], preferred_element_type=F32)
                low = jnp.dot(qb[:, 0:16].astype(BF16), ut_ref[:, cs], preferred_element_type=F32)
                x = th[b * HB:(b + 1) * HB, cs] - mu_ref[:, cs]
                sbuf[b * HB:(b + 1) * HB, cs] = (lik_weight * lik - x * lam_ref[:, cs] - low).astype(BF16)

            @pl.when(s == NUM_STEPS - 1)
            def _():
                out_s(b).start()

        score_phase(0, {3: [(stage_c, 3)], 6: [(stage_d, 2), (stage_b, 5)], 7: [(stage_b, 4)], 12: [(stage_d, 3)]})
        stage_e(2)
        stage_e(3)
        score_phase(1, {3: [(stage_c, 5)], 6: [(stage_c, 4)], 12: [(stage_d, 5)], 14: [(stage_d, 4)]})
        stage_e(5)
        stage_e(4)
        for p in range(3):
            small_k(p).wait_recv()
        ksum = (kall[0] + kall[1]) + (kall[2] + kall[3])
        kv[...] = jnp.broadcast_to(two_over_band * ksum[0:1, :], (128, N)).T
        kx[0:HB, HB:N] = kx[HB:N, 0:HB].astype(F32).T.astype(BF16)
        kx[:, N:2 * N] = (kx[:, 0:N].astype(F32) * -two_over_band).astype(BF16)
        for p in range(3):
            small_q(p).wait_send()
            small_g(p).wait_send()
            small_k(p).wait_send()

        @pl.when(s < NUM_STEPS - 1)
        def _():
            keep_block0().wait()
        return carry

    lax.fori_loop(0, NUM_STEPS, step, 0)
    k_copy = pltpu.make_async_copy(kx, k_out, out_sem.at[3])
    kv_copy = pltpu.make_async_copy(kv, kv_out, out_sem.at[4])
    k_copy.start()
    kv_copy.start()
    k_copy.wait()
    kv_copy.wait()
    out_theta().wait()
    out_s(0).wait()
    out_s(1).wait()


def last_kernel(gain, kx_hbm, kv_hbm, s_hbm, th_hbm, out_hbm, kx, kv, s, th, k_sem, s_sem, th_sem, out_sem):
    blocks = D // LW

    def copy(src, dst, sem, c):
        cs = pl.ds(pl.multiple_of(c * LW, LW), LW)
        return pltpu.make_async_copy(src.at[:, cs], dst.at[:, cs], sem.at[c])

    def fetch(c):
        copy(s_hbm, s, s_sem, c).start()
        copy(th_hbm, th, th_sem, c).start()

    k_copy = pltpu.make_async_copy(kx_hbm, kx, k_sem.at[0])
    kv_copy = pltpu.make_async_copy(kv_hbm, kv, k_sem.at[1])
    k_copy.start()
    kv_copy.start()
    for c in range(AHEAD):
        fetch(c)
    k_copy.wait()
    kv_copy.wait()

    def body(c, carry):
        copy(s_hbm, s, s_sem, c).wait()
        copy(th_hbm, th, th_sem, c).wait()

        @pl.when(c + AHEAD < blocks)
        def _():
            fetch(c + AHEAD)
        cs = pl.ds(pl.multiple_of(c * LW, LW), LW)
        t = th[:, cs]
        move = (jnp.dot(kx[:, 0:N], s[:, cs], preferred_element_type=F32)
                + jnp.dot(kx[:, N:2 * N], t.astype(BF16), preferred_element_type=F32))
        th[:, cs] = t + gain * (move + kv[:, 0:1] * t)
        copy(th, out_hbm, out_sem, c).start()
        return carry
    lax.fori_loop(0, blocks, body, 0)

    def drain(c, carry):
        copy(th, out_hbm, out_sem, c).wait()
        return carry
    lax.fori_loop(0, blocks, drain, 0)


def solution(mesh):
    feat = mesh.shape["feat"]
    dim_full = D * feat
    band = 2.0 * dim_full
    consts = (2.0 / math.sqrt(M * dim_full), 1.0 / band, 2.0 / band, dim_full / 4.0 / N)

    def local_run(particles, prec_diag, low_factor, prior_mean, data_mat, labels):
        targets = labels[None, :]
        vm = pl.BlockSpec(memory_space=pltpu.VMEM)
        anyspace = pl.BlockSpec(memory_space=pl.ANY)
        dma = pltpu.SemaphoreType.DMA
        th2, s2, k2, kv2 = pl.pallas_call(
            functools.partial(run_kernel, consts),
            out_shape=(jax.ShapeDtypeStruct((N, D), F32), jax.ShapeDtypeStruct((N, D), BF16),
                       jax.ShapeDtypeStruct((N, 2 * N), BF16), jax.ShapeDtypeStruct((N, 128), F32)),
            in_specs=[anyspace, vm, vm, vm, anyspace, vm],
            out_specs=(anyspace,) * 4,
            scratch_shapes=[
                pltpu.VMEM((N, D), F32), pltpu.VMEM((M, D), BF16), pltpu.VMEM((N, D), BF16), pltpu.VMEM((HB, D), BF16),
                pltpu.VMEM((N, D), BF16),
                pltpu.VMEM((6, HB, 512), F32), pltpu.VMEM((6, 128, 512), F32), pltpu.VMEM((6, 64, 512), F32),
                pltpu.VMEM((6, 64, 512), F32), pltpu.VMEM((N, M), BF16), pltpu.VMEM((N, 2 * N), BF16),
                pltpu.VMEM((N, 128), F32), pltpu.VMEM((16, N), F32), pltpu.VMEM((4, 16, N), F32),
                pltpu.VMEM((4, 8, N), F32), pltpu.VMEM((4, 8, N), F32), pltpu.VMEM((N, 128), F32),
                dma((8,)), dma((8,)), dma((5,)), dma((1,)),
                dma((6,)), dma((6,)), dma((6,)), dma((6,)), dma((6,)), dma((6,)), dma((6,)), dma((6,)),
                dma((3,)), dma((3,)), dma((3,)), dma((3,)), dma((3,)), dma((3,)),
            ],
            compiler_params=pltpu.CompilerParams(
                collective_id=0, has_side_effects=True, vmem_limit_bytes=VMEM_LIMIT),
        )(particles, prec_diag[None, :], low_factor.T, prior_mean[None, :], data_mat, targets)
        return pl.pallas_call(
            functools.partial(last_kernel, consts[3]),
            out_shape=jax.ShapeDtypeStruct((N, D), F32),
            in_specs=[anyspace] * 4,
            out_specs=anyspace,
            scratch_shapes=[
                pltpu.VMEM((N, 2 * N), BF16), pltpu.VMEM((N, 128), F32), pltpu.VMEM((N, D), BF16), pltpu.VMEM((N, D), F32),
                dma((2,)), dma((D // LW,)), dma((D // LW,)), dma((D // LW,)),
            ],
            compiler_params=pltpu.CompilerParams(vmem_limit_bytes=VMEM_LIMIT),
        )(k2, kv2, s2, th2)

    return jax.shard_map(
        local_run,
        mesh=mesh,
        in_specs=(P("ens", "feat"), P(("ens", "feat")), P(("ens", "feat"), None),
                  P(("ens", "feat")), P("ens", "feat"), P("ens")),
        out_specs=P("ens", "feat"),
        check_vma=False,
    )
```

```python
import functools
import math
import jax
import jax.numpy as jnp
from jax import lax
from jax.experimental import pallas as pl
from jax.experimental.pallas import tpu as pltpu
from jax.sharding import PartitionSpec as P

NUM_STEPS = 3
NT = (((1,), (1,)), ((), ()))
F32 = jnp.float32
BF16 = jnp.bfloat16
N = 512
HB = 256
D = 8192
M = 1024
CW = 2048
SW = 1024
SS = 512
NC = D // CW
LW = 1024
AHEAD = 4
VMEM_LIMIT = 67_043_328


def run_kernel(consts, th_hbm, lam_ref, ut_ref, mu_ref, a_hbm, y_ref,
               th_out, s_out, k_out, kv_out,
               th, a, tb, tn, sbuf, zbuf, ra, snd, rb, rbuf, kx, kv, qacc, qall, dall, kall, qt,
               ld_sem, a_sem, out_sem, tn_sem, as_sem, ar_sem, bs_sem, br_sem, cs_sem, cr_sem, ds_sem, dr_sem,
               qs_sem, qr_sem, gs_sem, gr_sem, ks_sem, kr_sem):
    lik_weight, inv_band, two_over_band, gain = consts
    me = lax.axis_index("feat")
    xx = me // 2
    cc = me % 2
    sib = xx * 2 + (1 - cc)
    far = (1 - xx) * 2 + cc
    diag_dev = (1 - xx) * 2 + (1 - cc)
    peers = (sib, far, diag_dev)

    def remote(src, dst, ssem, rsem, dev):
        return pltpu.make_async_remote_copy(
            src_ref=src, dst_ref=dst, send_sem=ssem, recv_sem=rsem,
            device_id={"feat": dev}, device_id_type=pl.DeviceIdType.MESH)

    def width(idx):
        return 256 if idx == 4 else 512

    def block(idx):
        return idx // 2 if idx < 4 else idx - 4

    def copy_a(idx):
        w = pl.ds(0, width(idx))
        return remote(zbuf.at[idx, pl.ds((1 - cc) * 128, 128), w], ra.at[idx, :, w],
                      as_sem.at[idx], ar_sem.at[idx], sib)

    def copy_b(idx):
        w = pl.ds(0, width(idx))
        return remote(snd.at[idx, :, w], rb.at[idx, :, w], bs_sem.at[idx], br_sem.at[idx], far)

    def region(idx, first, count):
        rows = pl.ds(block(idx) * HB + first, count)
        if idx >= 4:
            return kx.at[rows, pl.ds(0, width(idx))]
        return rbuf.at[rows, pl.ds((idx % 2) * 512, 512)]

    def copy_c(idx):
        r = region(idx, cc * 128 + xx * 64, 64)
        return remote(r, r, cs_sem.at[idx], cr_sem.at[idx], far)

    def copy_d(idx):
        r = region(idx, cc * 128, 128)
        return remote(r, r, ds_sem.at[idx], dr_sem.at[idx], sib)

    def small(buf, ssem, rsem, p):
        return remote(buf.at[me], buf.at[me], ssem.at[p], rsem.at[p], peers[p])

    small_q = functools.partial(small, qall, qs_sem, qr_sem)
    small_g = functools.partial(small, dall, gs_sem, gr_sem)
    small_k = functools.partial(small, kall, ks_sem, kr_sem)

    def stage_a(idx):
        copy_a(idx).start()

    def stage_b(idx):
        copy_a(idx).wait_recv()
        o = (1 - xx) * 64
        w = width(idx)
        snd[idx, :, 0:w] = zbuf[idx, pl.ds(cc * 128 + o, 64), 0:w] + ra[idx, pl.ds(o, 64), 0:w]
        copy_b(idx).start()

    def stage_c(idx):
        copy_b(idx).wait_recv()
        o = xx * 64
        w = width(idx)
        val = (zbuf[idx, pl.ds(cc * 128 + o, 64), 0:w] + ra[idx, pl.ds(o, 64), 0:w]) + rb[idx, :, 0:w]
        first = block(idx) * HB + cc * 128 + o
        if idx < 4:
            j = idx % 2
            res = y_ref[:, j * 512:(j + 1) * 512].astype(F32) - jax.nn.sigmoid(val)
            rbuf[pl.ds(first, 64), j * 512:(j + 1) * 512] = res.astype(BF16)
        else:
            if idx == 5:
                for p in range(3):
                    small_g(p).wait_recv()
            nj = ((dall[2 * xx] + dall[2 * xx + 1]) + (dall[2 * (1 - xx)] + dall[2 * (1 - xx) + 1]))[0:1, :]
            rid = lax.broadcasted_iota(jnp.int32, (64, N), 0) + first
            cid = lax.broadcasted_iota(jnp.int32, (64, N), 1)
            ni = jnp.sum(jnp.where(rid == cid, nj, 0.0), axis=1, keepdims=True)
            dist = jnp.maximum(ni + nj[:, 0:w] - 2.0 * val, 0.0)
            kern = jnp.exp(-dist * inv_band)
            kx[pl.ds(first, 64), 0:w] = kern.astype(BF16)
            col = jnp.sum(kern, axis=0, keepdims=True)
            if idx == 4:
                kall[me, :, 0:HB] += jnp.broadcast_to(col, (8, HB))
                for p in range(3):
                    small_k(p).start()
            else:
                kall[me, :, 0:HB] = jnp.broadcast_to(col[:, 0:HB], (8, HB))
                cross = jnp.sum(kern[:, 0:HB], axis=1, keepdims=True)
                placed = jnp.sum(jnp.where(rid[:, HB:] == cid[:, HB:], cross, 0.0), axis=0, keepdims=True)
                kall[me, :, HB:N] = jnp.broadcast_to(col[:, HB:N] + placed, (8, HB))
        copy_c(idx).start()
        copy_a(idx).wait_send()
        copy_b(idx).wait_send()

    def stage_d(idx):
        copy_c(idx).wait()
        copy_d(idx).start()

    def stage_e(idx):
        copy_d(idx).wait()

    def load_th(b, c):
        v = (pl.ds(b * HB, HB), pl.ds(pl.multiple_of(c * CW, CW), CW))
        return pltpu.make_async_copy(th_hbm.at[v], th.at[v], ld_sem.at[b * NC + c])

    def load_a(j, c):
        v = (pl.ds(j * 512 + c * 128, 128), slice(None))
        return pltpu.make_async_copy(a_hbm.at[v], a.at[v], a_sem.at[j * 4 + c])

    for c in range(NC):
        load_th(0, c).start()

    barrier = pltpu.get_barrier_semaphore()
    for p in peers:
        pl.semaphore_signal(barrier, inc=1, device_id={"feat": p}, device_id_type=pl.DeviceIdType.MESH)
    pl.semaphore_wait(barrier, 3)

    def out_theta():
        return pltpu.make_async_copy(th, th_out, out_sem.at[0])

    def out_s(b):
        v = (pl.ds(b * HB, HB), slice(None))
        return pltpu.make_async_copy(sbuf.at[v], s_out.at[v], out_sem.at[1 + b])

    def keep_block0():
        return pltpu.make_async_copy(tn, tb.at[pl.ds(0, HB), :], tn_sem.at[0])

    def new_block(b):
        return tn if b == 0 else tb.at[pl.ds(HB, HB), :]

    def step(s, carry):
        def at(cond, *todo):
            @pl.when(cond)
            def _():
                for f, i in todo:
                    f(i)

        def project():
            def body(c, carry):
                at(c == 1, (stage_b, 3))
                cs = pl.ds(pl.multiple_of(c * (2 * CW), CW), 2 * CW)
                xb = (th[:, cs] - mu_ref[:, cs]).astype(BF16)
                qacc[...] += lax.dot_general(ut_ref[:, cs], xb, NT, preferred_element_type=F32)
                return carry
            qacc[...] = jnp.zeros_like(qacc)
            lax.fori_loop(0, NC // 2, body, 0)

        def load_phase(b):
            def body(c, carry):
                load_th(b, c).wait()
                if b == 0:
                    load_a(0, c).start()
                for i in range(CW // SW):
                    cs = pl.ds(pl.multiple_of(c * CW + i * SW, SW), SW)
                    t = th[b * HB:(b + 1) * HB, cs]
                    new_block(b)[:, cs] = t.astype(BF16)
                return carry
            lax.fori_loop(0, NC, body, 0)

        def update_columns(b, cs):
            move = (jnp.dot(kx[b * HB:(b + 1) * HB, 0:N], sbuf[:, cs], preferred_element_type=F32)
                    + jnp.dot(kx[b * HB:(b + 1) * HB, N:2 * N], tb[:, cs], preferred_element_type=F32))
            t = th[b * HB:(b + 1) * HB, cs]
            t = t + gain * (move + kv[b * HB:(b + 1) * HB, 0:1] * t)
            th[b * HB:(b + 1) * HB, cs] = t
            new_block(b)[:, cs] = t.astype(BF16)

        def update_phase(b):
            if b == 0:
                def body(c, carry):
                    for i in range(4):
                        update_columns(b, pl.ds(pl.multiple_of(c * 4 * SW + i * SW, SW), SW))
                    return carry
                lax.fori_loop(0, D // (4 * SW), body, 0)
            else:
                for i in range(D // SW):
                    if i == 2:
                        stage_b(1)
                    if i == 6:
                        stage_c(0)
                    update_columns(b, slice(i * SW, (i + 1) * SW))

        def logits(b, j):
            zbuf[2 * b + j] = lax.dot_general(
                new_block(b)[...], a[j * 512:(j + 1) * 512, :], NT, preferred_element_type=F32)
            stage_a(2 * b + j)

        def gram(b, cols):
            g = lax.dot_general(new_block(b)[...], new_block(cols)[...], NT, preferred_element_type=F32)
            zbuf[4 + b, :, cols * HB:(cols + 1) * HB] = g
            if cols == b:
                eye = lax.broadcasted_iota(jnp.int32, (HB, HB), 0) == lax.broadcasted_iota(jnp.int32, (HB, HB), 1)
                row = jnp.sum(jnp.where(eye, g, 0.0), axis=0, keepdims=True)
                dall[me, :, b * HB:(b + 1) * HB] = jnp.broadcast_to(row, (8, HB))

        @pl.when(s == 0)
        def _():
            load_phase(0)
            gram(0, 0)
            for c in range(4):
                load_a(0, c).wait()
                load_a(1, c).start()

        @pl.when(s > 0)
        def _():
            update_phase(0)

        logits(0, 0)

        @pl.when(s == 0)
        def _():
            for c in range(4):
                load_a(1, c).wait()
                load_th(1, c).start()
        logits(0, 1)
        stage_b(0)

        @pl.when(s == 0)
        def _():
            load_phase(1)
            stage_b(1)

        @pl.when(s > 0)
        def _():
            update_phase(1)

        @pl.when(s == NUM_STEPS - 1)
        def _():
            out_theta().start()

        @pl.when(s < NUM_STEPS - 1)
        def _():
            keep_block0().start()

        logits(1, 0)
        at(s == 0, (stage_c, 0))
        at(s > 0, (stage_c, 1), (stage_d, 0))
        logits(1, 1)
        at(s == 0, (stage_c, 1))
        stage_b(2)
        project()
        qall[me] = qacc[...]
        for p in range(3):
            small_q(p).start()
        gram(1, 0)
        at(s == 0, (stage_d, 0))
        at(s > 0, (stage_d, 1))
        gram(1, 1)
        stage_a(5)
        stage_c(2)
        at(s == 0, (stage_d, 1))

        @pl.when(s > 0)
        def _():
            gram(0, 0)
        stage_a(4)
        for p in range(3):
            small_g(p).start()
        stage_e(0)
        stage_e(1)
        for p in range(3):
            small_q(p).wait_recv()
        qsum = (qall[0] + qall[1]) + (qall[2] + qall[3])
        qt[...] = jnp.concatenate([qsum, jnp.zeros((112, N), F32)], axis=0).T

        def score_phase(b, events):
            rr = rbuf.at[pl.ds(b * HB, HB), :]
            qb = qt.at[pl.ds(b * HB, HB), pl.ds(0, 128)]
            for i in range(D // SS):
                for f, idx in events.get(i, ()):
                    f(idx)
                cs = slice(i * SS, (i + 1) * SS)
                lik = jnp.dot(rr[...], a[:, cs], preferred_element_type=F32)
                low = jnp.dot(qb[:, 0:16].astype(BF16), ut_ref[:, cs], preferred_element_type=F32)
                x = th[b * HB:(b + 1) * HB, cs] - mu_ref[:, cs]
                sbuf[b * HB:(b + 1) * HB, cs] = (lik_weight * lik - x * lam_ref[:, cs] - low).astype(BF16)

            @pl.when(s == NUM_STEPS - 1)
            def _():
                out_s(b).start()

        score_phase(0, {3: [(stage_c, 3)], 6: [(stage_d, 2), (stage_b, 5)], 7: [(stage_b, 4)], 12: [(stage_d, 3)]})
        stage_e(2)
        stage_e(3)
        score_phase(1, {3: [(stage_c, 5)], 6: [(stage_c, 4)], 12: [(stage_d, 5)], 14: [(stage_d, 4)]})
        stage_e(5)
        stage_e(4)
        for p in range(3):
            small_k(p).wait_recv()
        ksum = (kall[0] + kall[1]) + (kall[2] + kall[3])
        kv[...] = jnp.broadcast_to(two_over_band * ksum[0:1, :], (128, N)).T
        kx[0:HB, HB:N] = kx[HB:N, 0:HB].astype(F32).T.astype(BF16)
        kx[:, N:2 * N] = (kx[:, 0:N].astype(F32) * -two_over_band).astype(BF16)
        for p in range(3):
            small_q(p).wait_send()
            small_g(p).wait_send()
            small_k(p).wait_send()

        @pl.when(s < NUM_STEPS - 1)
        def _():
            keep_block0().wait()
        return carry

    lax.fori_loop(0, NUM_STEPS, step, 0)
    k_copy = pltpu.make_async_copy(kx, k_out, out_sem.at[3])
    kv_copy = pltpu.make_async_copy(kv, kv_out, out_sem.at[4])
    k_copy.start()
    kv_copy.start()
    k_copy.wait()
    kv_copy.wait()
    out_theta().wait()
    out_s(0).wait()
    out_s(1).wait()


def last_kernel(gain, kx_hbm, kv_hbm, s_hbm, th_hbm, out_hbm, kx, kv, s, th, k_sem, s_sem, th_sem, out_sem):
    blocks = D // LW

    def copy(src, dst, sem, c):
        cs = pl.ds(pl.multiple_of(c * LW, LW), LW)
        return pltpu.make_async_copy(src.at[:, cs], dst.at[:, cs], sem.at[c])

    def fetch(c):
        copy(s_hbm, s, s_sem, c).start()
        copy(th_hbm, th, th_sem, c).start()

    k_copy = pltpu.make_async_copy(kx_hbm, kx, k_sem.at[0])
    kv_copy = pltpu.make_async_copy(kv_hbm, kv, k_sem.at[1])
    k_copy.start()
    kv_copy.start()
    for c in range(AHEAD):
        fetch(c)
    k_copy.wait()
    kv_copy.wait()

    def body(c, carry):
        copy(s_hbm, s, s_sem, c).wait()
        copy(th_hbm, th, th_sem, c).wait()

        @pl.when(c + AHEAD < blocks)
        def _():
            fetch(c + AHEAD)
        cs = pl.ds(pl.multiple_of(c * LW, LW), LW)
        t = th[:, cs]
        move = (jnp.dot(kx[:, 0:N], s[:, cs], preferred_element_type=F32)
                + jnp.dot(kx[:, N:2 * N], t.astype(BF16), preferred_element_type=F32))
        th[:, cs] = t + gain * (move + kv[:, 0:1] * t)
        copy(th, out_hbm, out_sem, c).start()
        return carry
    lax.fori_loop(0, blocks, body, 0)

    def drain(c, carry):
        copy(th, out_hbm, out_sem, c).wait()
        return carry
    lax.fori_loop(0, blocks, drain, 0)


def solution(mesh):
    feat = mesh.shape["feat"]
    dim_full = D * feat
    band = 2.0 * dim_full
    consts = (2.0 / math.sqrt(M * dim_full), 1.0 / band, 2.0 / band, dim_full / 4.0 / N)

    def local_run(particles, prec_diag, low_factor, prior_mean, data_mat, labels):
        targets = labels[None, :]
        vm = pl.BlockSpec(memory_space=pltpu.VMEM)
        anyspace = pl.BlockSpec(memory_space=pl.ANY)
        dma = pltpu.SemaphoreType.DMA
        th2, s2, k2, kv2 = pl.pallas_call(
            functools.partial(run_kernel, consts),
            out_shape=(jax.ShapeDtypeStruct((N, D), F32), jax.ShapeDtypeStruct((N, D), BF16),
                       jax.ShapeDtypeStruct((N, 2 * N), BF16), jax.ShapeDtypeStruct((N, 128), F32)),
            in_specs=[anyspace, vm, vm, vm, anyspace, vm],
            out_specs=(anyspace,) * 4,
            scratch_shapes=[
                pltpu.VMEM((N, D), F32), pltpu.VMEM((M, D), BF16), pltpu.VMEM((N, D), BF16), pltpu.VMEM((HB, D), BF16),
                pltpu.VMEM((N, D), BF16),
                pltpu.VMEM((6, HB, 512), F32), pltpu.VMEM((6, 128, 512), F32), pltpu.VMEM((6, 64, 512), F32),
                pltpu.VMEM((6, 64, 512), F32), pltpu.VMEM((N, M), BF16), pltpu.VMEM((N, 2 * N), BF16),
                pltpu.VMEM((N, 128), F32), pltpu.VMEM((16, N), F32), pltpu.VMEM((4, 16, N), F32),
                pltpu.VMEM((4, 8, N), F32), pltpu.VMEM((4, 8, N), F32), pltpu.VMEM((N, 128), F32),
                dma((8,)), dma((8,)), dma((5,)), dma((1,)),
                dma((6,)), dma((6,)), dma((6,)), dma((6,)), dma((6,)), dma((6,)), dma((6,)), dma((6,)),
                dma((3,)), dma((3,)), dma((3,)), dma((3,)), dma((3,)), dma((3,)),
            ],
            compiler_params=pltpu.CompilerParams(
                collective_id=0, has_side_effects=True, vmem_limit_bytes=VMEM_LIMIT),
        )(particles, prec_diag[None, :], low_factor.T, prior_mean[None, :], data_mat, targets)
        return pl.pallas_call(
            functools.partial(last_kernel, consts[3]),
            out_shape=jax.ShapeDtypeStruct((N, D), F32),
            in_specs=[anyspace] * 4,
            out_specs=anyspace,
            scratch_shapes=[
                pltpu.VMEM((N, 2 * N), BF16), pltpu.VMEM((N, 128), F32), pltpu.VMEM((N, D), BF16), pltpu.VMEM((N, D), F32),
                dma((2,)), dma((D // LW,)), dma((D // LW,)), dma((D // LW,)),
            ],
            compiler_params=pltpu.CompilerParams(vmem_limit_bytes=VMEM_LIMIT),
        )(k2, kv2, s2, th2)

    return jax.shard_map(
        local_run,
        mesh=mesh,
        in_specs=(P("ens", "feat"), P(("ens", "feat")), P(("ens", "feat"), None),
                  P(("ens", "feat")), P("ens", "feat"), P("ens")),
        out_specs=P("ens", "feat"),
        check_vma=False,
    )
```
